32 devices in a mesh: dp: 8 (over z, y), mp: 4 (over x, core).
Axes of the slice: x: 2, y: 2, z: 4, core: 2. Of those that a mesh axis runs over, the one named last changes fastest.
Arguments:
- gradient: bfloat16 [8, 64, 14336], P('dp', None, 'mp'), may hold values from -6 to 6
- momentum: float32 [8, 64, 14336], P('dp', None, 'mp'), may hold values from -6 to 6
- weights: float32 [64, 14336], P(None, 'mp'), may hold values from -6 to 6
- positions: int32 [8, 1, 224, 32], P('dp', None, 'mp'), may hold values from 0 to 4095, as said below
Outputs:
- new_momentum: float32 [8, 64, 14336], P('dp', None, 'mp')
- new_weights: float32 [64, 14336], P(None, 'mp')
The draws below stay inside these ranges and needn't reach their ends.
Inputs may be any that keep to these rules, and one draw needn't show every extreme that they name: Within one span of one replica the 32 positions are all different.
All inputs are finite; a program needn't handle non-finite values.
Results may differ from the reference program's by a relative error of at most 0.0003.
Values sent between devices are 32-bit elements; how exact they have to be, the bound alone decides.
A program may use at most 64 MiB of HBM per device.

```python
import jax
import jax.numpy as jnp
from jax import lax

FF = 14336
BANDS = 1
K = 32
REPLICAS = 8
COLCH = 224


def draw_positions(key, part):
    scores = jax.random.randint(key, (REPLICAS, BANDS, FF // 64, 4096), 0, 262144, dtype=jnp.int32)
    scores = scores * 4096 + jnp.arange(4096, dtype=jnp.int32)
    chosen = jax.lax.top_k(scores, K)[1]
    return chosen.astype(jnp.int32)


def levels(own_key, dims, split, least, top_value):
    level, own = 1.0, jax.random.fold_in(own_key, 6)
    for dim, blocks in split:
        heights = jnp.exp(jax.random.uniform(jax.random.fold_in(own, dim), (blocks,), jnp.float32, least / len(split), top_value / len(split)))
        level = level * jnp.repeat(heights, dims[dim] // blocks).reshape([-1 if axis == dim else 1 for axis in range(len(dims))])
    return level


def normal_values(rng, extent, scale, most, shards=(), held_as=jnp.bfloat16):
    result = scale * jax.random.normal(rng, extent, jnp.float32)
    if shards:
        result = result * levels(rng, extent, shards, -0.22, 0.18)
    return jnp.clip(result, -most, most).astype(held_as)


def setup_inputs(seed: int = 0) -> dict:
    splits = jax.random.split(jax.random.key(seed), 5)
    gradient = normal_values(splits[0], (REPLICAS, 64 * BANDS, FF), 1.0, 6.0, ((0, 8), (2, 4)))
    momentum = normal_values(splits[1], (REPLICAS, 64 * BANDS, FF), 1.0, 6.0, ((0, 8), (2, 4)), jnp.float32)
    weights = normal_values(splits[2], (64 * BANDS, FF), 1.0, 6.0, ((1, 4),), jnp.float32)
    positions = draw_positions(jax.random.fold_in(splits[4], 71), 0)
    return {"gradient": gradient, "momentum": momentum, "weights": weights, "positions": positions}


def dct_table():
    column = jnp.arange(64, dtype=jnp.float32)
    freq = column[:, None]
    factor = jnp.where(freq == 0, jnp.sqrt(jnp.float32(1.0 / 64)), jnp.sqrt(jnp.float32(2.0 / 64)))
    return factor * jnp.cos(jnp.pi * (2.0 * column[None, :] + 1.0) * freq / 128.0)

def reference(gradient, momentum, weights, positions):
    table = dct_table()
    rows_all = 64 * BANDS
    band_index = jnp.arange(BANDS, dtype=jnp.int32)[:, None, None]
    span_index = jnp.arange(COLCH, dtype=jnp.int32)[None, :, None]

    def one_replica(carry, inputs):
        grad_one, mom_one, pos_one = inputs
        summed = 0.9 * mom_one + grad_one.astype(jnp.float32)
        blocks = summed.reshape(BANDS, 64, COLCH, 64)
        coefs = jnp.einsum('kr,brcs,ls->bckl', table, blocks, table, precision=lax.Precision.HIGHEST)
        flatten = coefs.reshape(BANDS, COLCH, 4096)
        picked = jnp.take_along_axis(flatten, pos_one, axis=2)
        own = jnp.zeros((BANDS, COLCH, 4096), jnp.float32).at[band_index, span_index, pos_one].add(picked)
        back = jnp.einsum('kr,bckl,ls->brcs', table, own.reshape(BANDS, COLCH, 64, 64), table, precision=lax.Precision.HIGHEST)
        return (carry + own, summed - back.reshape(rows_all, FF))
    start = jnp.zeros((BANDS, COLCH, 4096), jnp.float32)
    aggregate, new_momentum = lax.scan(one_replica, start, (gradient, momentum, positions))
    update = jnp.einsum('kr,bckl,ls->brcs', table, aggregate.reshape(BANDS, COLCH, 64, 64), table, precision=lax.Precision.HIGHEST)
    update = update.reshape(rows_all, FF)
    meansq = jnp.mean(update * update)
    new_weights = weights - update / jnp.sqrt(meansq + 1.0)
    return (new_momentum, new_weights)
```

```python
import functools

import jax
import jax.numpy as jnp
import numpy as np
from jax import lax
from jax.experimental import pallas as pl
from jax.experimental.pallas import tpu as pltpu
from jax.sharding import PartitionSpec as P

QUAD = 256
LISTED = 128
F32 = jnp.float32
BF16 = jnp.bfloat16


def dct_table():
    column = np.arange(64, dtype=np.float64)
    freq = column[:, None]
    factor = np.where(freq == 0, np.sqrt(1.0 / 64), np.sqrt(2.0 / 64))
    return factor * np.cos(np.pi * (2.0 * column[None, :] + 1.0) * freq / 128.0)


def halves(table):
    high = np.asarray(table, np.float32).astype(jnp.bfloat16)
    low = np.asarray(table - high.astype(np.float64), np.float32).astype(jnp.bfloat16)
    return high, low


def side_tables():
    table = dct_table()
    rows, columns = [], []
    for row, column in ((table, table.T), (table.T, table)):
        high, low = halves(row)
        rows.append(np.concatenate([high, low, high, low], axis=1))
        high, low = halves(np.kron(np.eye(4), column))
        columns.append(np.concatenate([high, high, low], axis=0))
    return np.stack(rows), np.stack(columns)


def split(value):
    high = value.astype(BF16)
    return high, (value - high.astype(F32)).astype(BF16)


def dot(a, b):
    return jnp.dot(a, b, preferred_element_type=F32)


def dot_t(a, b):
    return lax.dot_general(a, b, (((1,), (1,)), ((), ())), preferred_element_type=F32)


def row_transform(table, value):
    high, low = split(value)
    return dot(table, jnp.concatenate([high, high, low, low], axis=0))


def column_transform(high, low, table):
    return dot(jnp.concatenate([high, low, high], axis=1), table)


def hot(freq, rows):
    return jnp.where(lax.broadcasted_iota(jnp.int32, (rows, LISTED), 0) == freq, 1.0, 0.0)


def targets(places):
    lane = lax.broadcasted_iota(jnp.int32, places.shape, 1)
    return places // 64, places % 64 + lane // 32 * 64


def loop(count, body):
    if count <= 16:
        for step in range(count):
            body(step)
    else:
        lax.fori_loop(0, count, lambda step, carry: (body(step), carry)[1], 0)


def kernel(
    replicas, parts, entries,
    gradient_ref, momentum_ref, weights_ref, places_ref, rows_ref, columns_ref,
    out_momentum_ref, out_weights_ref,
    grad, mom, wts, summed, high, low, coefs, field, update, lists, squares,
    in_sem, out_sem, send_sem, recv_sem, square_send, square_recv,
):
    me, mine = lax.axis_index("dp"), lax.axis_index("mp")
    width = summed.shape[1]
    quads = width // QUAD

    loads = [
        pltpu.make_async_copy(source, target, in_sem.at[index])
        for index, (source, target) in enumerate(
            ((gradient_ref.at[0], grad), (momentum_ref.at[0], mom), (weights_ref, wts))
        )
    ]
    for load in loads:
        load.start()

    barrier = pltpu.get_barrier_semaphore()

    def greet_replica(step):
        pl.semaphore_signal(
            barrier, inc=1, device_id={"dp": lax.rem(me + step + 1, replicas)},
            device_id_type=pl.DeviceIdType.MESH,
        )

    def greet_part(step):
        pl.semaphore_signal(
            barrier, inc=1, device_id={"mp": lax.rem(mine + step + 1, parts)},
            device_id_type=pl.DeviceIdType.MESH,
        )

    loop(replicas - 1, greet_replica)
    loop(parts - 1, greet_part)

    def block(index):
        return pl.ds(index * QUAD, QUAD)

    def rows(index):
        return pl.ds(index * 64, 64)

    loads[0].wait()
    loads[1].wait()
    for index in range(quads):
        value = 0.9 * mom[:, block(index)] + grad[:, block(index)].astype(F32)
        summed[:, block(index)] = value
        high[rows(index), :], low[rows(index), :] = split(row_transform(rows_ref[0], value))
    coefs[...] = column_transform(high[...], low[...], columns_ref[0])

    places = jnp.concatenate(
        [places_ref[0, 0, pl.ds(part, quads, stride=4), :] for part in range(4)], axis=1
    )
    lists[me, 0, 0:quads, :] = places.astype(F32)
    row_freqs, column_spots = targets(places)
    for index in range(quads):
        row_hot = hot(row_freqs[index : index + 1, :], 64)
        column_hot = hot(column_spots[index : index + 1, :], QUAD).astype(BF16)
        value = coefs[rows(index), :]
        found = dot(jnp.concatenate(split(value), axis=0), column_hot)
        found = (found[:64, :] + found[64:, :]) * row_hot
        lists[me, 1, index : index + 1, :] = jnp.sum(found, axis=0, keepdims=True)
        own = value * dot_t(row_hot.astype(BF16), column_hot)
        high[rows(index), :], low[rows(index), :] = split(own)

    pl.semaphore_wait(barrier, replicas - 1 + parts - 1)

    def list_copy(step, slot):
        return pltpu.make_async_remote_copy(
            src_ref=lists.at[slot], dst_ref=lists.at[slot],
            send_sem=send_sem.at[step], recv_sem=recv_sem.at[slot],
            device_id={"dp": lax.rem(me + step + 1, replicas)},
            device_id_type=pl.DeviceIdType.MESH,
        )

    loop(replicas - 1, lambda step: list_copy(step, me).start())

    field[...] = column_transform(high[...], low[...], columns_ref[1])
    for index in range(quads):
        back = row_transform(rows_ref[1], field[rows(index), :])
        summed[:, block(index)] = summed[:, block(index)] - back
    store_momentum = pltpu.make_async_copy(summed, out_momentum_ref.at[0], out_sem.at[0])
    store_momentum.start()

    def receive(step):
        list_copy(step, lax.rem(me + replicas - step - 1, replicas)).wait_recv()

    loop(replicas - 1, receive)

    group = int(np.gcd(replicas, 8))
    square = jnp.zeros((8, QUAD), F32)

    def add_group(start, index):
        lefts_high, lefts_low, rights = [], [], []
        for member in range(group):
            row_freq, spots = targets(lists[start + member, 0, index : index + 1, :].astype(jnp.int32))
            left = hot(row_freq, 64) * lists[start + member, 1, index : index + 1, :]
            left_high, left_low = split(left)
            lefts_high.append(left_high)
            lefts_low.append(left_low)
            rights.append(hot(spots, QUAD).astype(BF16))
        left = jnp.concatenate(
            [jnp.concatenate(lefts_high, axis=1), jnp.concatenate(lefts_low, axis=1)], axis=0
        )
        result = dot_t(left, jnp.concatenate(rights, axis=1))
        return result[:64, :] + result[64:, :]

    for index in range(quads):
        total = add_group(0, index)
        if replicas > group:
            total = lax.fori_loop(
                1, replicas // group, lambda step, acc: acc + add_group(step * group, index), total
            )
        square = square + jnp.sum((total * total).reshape(8, 8, QUAD), axis=0)
        high[rows(index), :], low[rows(index), :] = split(total)

    squares[mine, :, :] = square

    def square_copy(step, slot):
        return pltpu.make_async_remote_copy(
            src_ref=squares.at[slot], dst_ref=squares.at[slot],
            send_sem=square_send.at[step], recv_sem=square_recv.at[slot],
            device_id={"mp": lax.rem(mine + step + 1, parts)},
            device_id_type=pl.DeviceIdType.MESH,
        )

    loop(parts - 1, lambda step: square_copy(step, mine).start())

    field[...] = column_transform(high[...], low[...], columns_ref[1])
    for index in range(quads):
        update[:, block(index)] = row_transform(rows_ref[1], field[rows(index), :])

    loop(
        parts - 1,
        lambda step: square_copy(step, lax.rem(mine + parts - step - 1, parts)).wait_recv(),
    )
    loads[2].wait()
    meansq = jnp.sum(jnp.sum(squares[...], axis=0)) / entries
    factor = lax.rsqrt(jnp.full((1, QUAD), meansq + 1.0, F32))
    for index in range(quads):
        update[:, block(index)] = wts[:, block(index)] - update[:, block(index)] * factor
    store_weights = pltpu.make_async_copy(update, out_weights_ref, out_sem.at[1])
    store_weights.start()
    loop(replicas - 1, lambda step: list_copy(step, me).wait_send())
    loop(parts - 1, lambda step: square_copy(step, mine).wait_send())
    store_momentum.wait()
    store_weights.wait()


def local(replicas, parts, gradient, momentum, weights, positions):
    height, width = weights.shape
    quads = width // QUAD
    row_tables, column_tables = side_tables()
    anywhere = pl.BlockSpec(memory_space=pl.ANY)
    vmem = pl.BlockSpec(memory_space=pltpu.VMEM)
    listed = -(-quads // 8) * 8
    return pl.pallas_call(
        functools.partial(kernel, replicas, parts, float(height * width * parts)),
        out_shape=(
            jax.ShapeDtypeStruct(momentum.shape, F32),
            jax.ShapeDtypeStruct(weights.shape, F32),
        ),
        in_specs=[anywhere, anywhere, anywhere, vmem, vmem, vmem],
        out_specs=(anywhere, anywhere),
        scratch_shapes=[
            pltpu.VMEM((height, width), BF16),
            pltpu.VMEM((height, width), F32),
            pltpu.VMEM((height, width), F32),
            pltpu.VMEM((height, width), F32),
            pltpu.VMEM((quads * 64, QUAD), BF16),
            pltpu.VMEM((quads * 64, QUAD), BF16),
            pltpu.VMEM((quads * 64, QUAD), F32),
            pltpu.VMEM((quads * 64, QUAD), F32),
            pltpu.VMEM((height, width), F32),
            pltpu.VMEM((replicas, 2, listed, LISTED), F32),
            pltpu.VMEM((parts, 8, QUAD), F32),
            pltpu.SemaphoreType.DMA((3,)),
            pltpu.SemaphoreType.DMA((2,)),
            pltpu.SemaphoreType.DMA((replicas,)),
            pltpu.SemaphoreType.DMA((replicas,)),
            pltpu.SemaphoreType.DMA((parts,)),
            pltpu.SemaphoreType.DMA((parts,)),
        ],
        compiler_params=pltpu.CompilerParams(collective_id=0, has_side_effects=True),
    )(gradient, momentum, weights, positions, jnp.asarray(row_tables), jnp.asarray(column_tables))


def solution(mesh):
    placed = (P("dp", None, "mp"), P("dp", None, "mp"), P(None, "mp"), P("dp", None, "mp", None))
    return jax.shard_map(
        functools.partial(local, mesh.shape["dp"], mesh.shape["mp"]),
        mesh=mesh,
        in_specs=placed,
        out_specs=(P("dp", None, "mp"), P(None, "mp")),
        check_vma=False,
    )
```

```python
import functools

import jax
import jax.numpy as jnp
import numpy as np
from jax import lax
from jax.experimental import pallas as pl
from jax.experimental.pallas import tpu as pltpu
from jax.sharding import PartitionSpec as P

QUAD = 256
LISTED = 128
F32 = jnp.float32
BF16 = jnp.bfloat16


def dct_table():
    column = np.arange(64, dtype=np.float64)
    freq = column[:, None]
    factor = np.where(freq == 0, np.sqrt(1.0 / 64), np.sqrt(2.0 / 64))
    return factor * np.cos(np.pi * (2.0 * column[None, :] + 1.0) * freq / 128.0)


def halves(table):
    high = np.asarray(table, np.float32).astype(jnp.bfloat16)
    low = np.asarray(table - high.astype(np.float64), np.float32).astype(jnp.bfloat16)
    return high, low


def side_tables():
    table = dct_table()
    rows = []
    for row in (table, table.T):
        high, low = halves(row)
        rows.append(np.concatenate([high, low, high, low], axis=1))
    return np.stack(rows), np.stack(halves(np.kron(np.eye(4), table)))


def split(value):
    high = value.astype(BF16)
    return high, (value - high.astype(F32)).astype(BF16)


def dot(a, b):
    return jnp.dot(a, b, preferred_element_type=F32)


def dot_t(a, b):
    return lax.dot_general(a, b, (((1,), (1,)), ((), ())), preferred_element_type=F32)


def row_transform(table, value):
    high, low = split(value)
    return dot(table, jnp.concatenate([high, high, low, low], axis=0))


def forward_columns(high, low, table_ref):
    table = jnp.concatenate([table_ref[0], table_ref[0], table_ref[1]], axis=1)
    return dot_t(jnp.concatenate([high, low, high], axis=1), table)


def inverse_columns(high, low, table_ref):
    table = jnp.concatenate([table_ref[0], table_ref[0], table_ref[1]], axis=0)
    return dot(jnp.concatenate([high, low, high], axis=1), table)


def counting(rows):
    return lax.broadcasted_iota(jnp.int32, (rows, LISTED), 0).astype(F32).astype(BF16).reshape(-1, 16, LISTED)


def spread(row):
    return jnp.broadcast_to(row, (16, LISTED)).astype(BF16)[None]


def hot(freq, value, count):
    zero = jnp.zeros((), BF16)
    return jnp.where(count == freq, value, zero).reshape(-1, LISTED)


def targets(places):
    lane = lax.broadcasted_iota(jnp.int32, places.shape, 1)
    return (places // 64).astype(F32), (places % 64 + lane // 32 * 64).astype(F32)


def loop(count, body):
    if count <= 16:
        for step in range(count):
            body(step)
    else:
        lax.fori_loop(0, count, lambda step, carry: (body(step), carry)[1], 0)


def kernel(
    replicas, parts, entries,
    gradient_ref, momentum_ref, weights_ref, places_hbm, rows_hbm, columns_hbm,
    summed, update,
    grad, mom, wts, places_ref, rows_ref, columns_ref, flipped, high, low, coefs, field, lists, squares,
    in_sem, send_sem, recv_sem, square_send, square_recv,
):
    me, mine = lax.axis_index("dp"), lax.axis_index("mp")
    width = summed.shape[1]
    quads = width // QUAD

    loads = [
        pltpu.make_async_copy(source, target, in_sem.at[index])
        for index, (source, target) in enumerate(
            (
                (gradient_ref.at[0], grad), (momentum_ref.at[0], mom), (rows_hbm, rows_ref),
                (columns_hbm, columns_ref), (places_hbm.at[0, 0], places_ref), (weights_ref, wts),
            )
        )
    ]
    for load in loads:
        load.start()

    barrier = pltpu.get_barrier_semaphore()

    def greet_replica(step):
        pl.semaphore_signal(
            barrier, inc=1, device_id={"dp": lax.rem(me + step + 1, replicas)},
            device_id_type=pl.DeviceIdType.MESH,
        )

    def greet_part(step):
        pl.semaphore_signal(
            barrier, inc=1, device_id={"mp": lax.rem(mine + step + 1, parts)},
            device_id_type=pl.DeviceIdType.MESH,
        )

    loop(replicas - 1, greet_replica)
    loop(parts - 1, greet_part)

    def block(index):
        return pl.ds(index * QUAD, QUAD)

    def rows(index):
        return pl.ds(index * 64, 64)

    count_rows, count_columns = counting(64), counting(QUAD)
    one = jnp.ones((1, 16, LISTED), BF16)

    for load in loads[:3]:
        load.wait()
    for index in range(quads):
        value = 0.9 * mom[:, block(index)] + grad[:, block(index)].astype(F32)
        summed[:, block(index)] = value
        high[rows(index), :], low[rows(index), :] = split(row_transform(rows_ref[0], value))
    loads[3].wait()
    coefs[...] = forward_columns(high[...], low[...], columns_ref)

    loads[4].wait()
    flipped[...] = jnp.transpose(places_ref[...])
    places = jnp.concatenate(
        [flipped[pl.ds(part, quads, stride=4), :] for part in range(4)], axis=1
    )
    lists[me, 0, 0:quads, :] = places.astype(F32)
    row_freqs, column_spots = targets(places)
    for index in range(quads):
        row_hot = hot(spread(row_freqs[index : index + 1, :]), one, count_rows)
        column_hot = hot(spread(column_spots[index : index + 1, :]), one, count_columns)
        value = coefs[rows(index), :]
        found = dot(jnp.concatenate(split(value), axis=0), column_hot)
        found = (found[:64, :] + found[64:, :]) * row_hot.astype(F32)
        lists[me, 1, index : index + 1, :] = jnp.sum(found, axis=0, keepdims=True)
        own = value * dot_t(row_hot, column_hot)
        high[rows(index), :], low[rows(index), :] = split(own)

    pl.semaphore_wait(barrier, replicas - 1 + parts - 1)

    def list_copy(step, slot):
        return pltpu.make_async_remote_copy(
            src_ref=lists.at[slot], dst_ref=lists.at[slot],
            send_sem=send_sem.at[step], recv_sem=recv_sem.at[slot],
            device_id={"dp": lax.rem(me + step + 1, replicas)},
            device_id_type=pl.DeviceIdType.MESH,
        )

    loop(replicas - 1, lambda step: list_copy(step, me).start())

    field[...] = inverse_columns(high[...], low[...], columns_ref)
    for index in range(quads):
        back = row_transform(rows_ref[1], field[rows(index), :])
        summed[:, block(index)] = summed[:, block(index)] - back

    def receive(step):
        list_copy(step, lax.rem(me + replicas - step - 1, replicas)).wait_recv()

    loop(replicas - 1, receive)

    group = int(np.gcd(replicas, 8))
    square = jnp.zeros((8, QUAD), F32)

    def add_group(start, index):
        lefts_high, lefts_low, rights = [], [], []
        for member in range(group):
            row_freq, spots = targets(lists[start + member, 0, index : index + 1, :].astype(jnp.int32))
            value_high, value_low = split(
                jnp.broadcast_to(lists[start + member, 1, index : index + 1, :], (16, LISTED))
            )
            row_freq = spread(row_freq)
            lefts_high.append(hot(row_freq, value_high[None], count_rows))
            lefts_low.append(hot(row_freq, value_low[None], count_rows))
            rights.append(hot(spread(spots), one, count_columns))
        left = jnp.concatenate(
            [jnp.concatenate(lefts_high, axis=1), jnp.concatenate(lefts_low, axis=1)], axis=0
        )
        result = dot_t(left, jnp.concatenate(rights, axis=1))
        return result[:64, :] + result[64:, :]

    for index in range(quads):
        total = add_group(0, index)
        if replicas > group:
            total = lax.fori_loop(
                1, replicas // group, lambda step, acc: acc + add_group(step * group, index), total
            )
        square = square + jnp.sum((total * total).reshape(8, 8, QUAD), axis=0)
        high[rows(index), :], low[rows(index), :] = split(total)

    squares[mine, :, :] = square

    def square_copy(step, slot):
        return pltpu.make_async_remote_copy(
            src_ref=squares.at[slot], dst_ref=squares.at[slot],
            send_sem=square_send.at[step], recv_sem=square_recv.at[slot],
            device_id={"mp": lax.rem(mine + step + 1, parts)},
            device_id_type=pl.DeviceIdType.MESH,
        )

    loop(parts - 1, lambda step: square_copy(step, mine).start())

    field[...] = inverse_columns(high[...], low[...], columns_ref)
    for index in range(quads):
        update[:, block(index)] = row_transform(rows_ref[1], field[rows(index), :])

    loop(
        parts - 1,
        lambda step: square_copy(step, lax.rem(mine + parts - step - 1, parts)).wait_recv(),
    )
    loads[5].wait()
    meansq = jnp.sum(jnp.sum(squares[...], axis=0)) / entries
    factor = lax.rsqrt(jnp.full((1, QUAD), meansq + 1.0, F32))
    for index in range(quads):
        update[:, block(index)] = wts[:, block(index)] - update[:, block(index)] * factor
    loop(replicas - 1, lambda step: list_copy(step, me).wait_send())
    loop(parts - 1, lambda step: square_copy(step, mine).wait_send())


def deliver(summed, update, out_momentum_ref, out_weights_ref, out_sem):
    stores = (
        pltpu.make_async_copy(summed, out_momentum_ref.at[0], out_sem.at[0]),
        pltpu.make_async_copy(update, out_weights_ref, out_sem.at[1]),
    )
    for store in stores:
        store.start()
    for store in stores:
        store.wait()


def local(replicas, parts, gradient, momentum, weights, positions):
    height, width = weights.shape
    quads = width // QUAD
    row_tables, column_tables = side_tables()
    anywhere = pl.BlockSpec(memory_space=pl.ANY)
    vmem = pl.BlockSpec(memory_space=pltpu.VMEM)
    listed = -(-quads // 8) * 8
    entries = positions.shape[-1]
    results = pl.pallas_call(
        functools.partial(kernel, replicas, parts, float(height * width * parts)),
        out_shape=(
            jax.ShapeDtypeStruct(weights.shape, F32),
            jax.ShapeDtypeStruct(weights.shape, F32),
        ),
        in_specs=[pl.BlockSpec(memory_space=pltpu.HBM)] * 6,
        out_specs=(vmem, vmem),
        scratch_shapes=[
            pltpu.VMEM((height, width), BF16),
            pltpu.VMEM((height, width), F32),
            pltpu.VMEM((height, width), F32),
            pltpu.VMEM((entries, 4 * quads), jnp.int32),
            pltpu.VMEM(row_tables.shape, BF16),
            pltpu.VMEM(column_tables.shape, BF16),
            pltpu.VMEM((4 * quads, entries), jnp.int32),
            pltpu.VMEM((quads * 64, QUAD), BF16),
            pltpu.VMEM((quads * 64, QUAD), BF16),
            pltpu.VMEM((quads * 64, QUAD), F32),
            pltpu.VMEM((quads * 64, QUAD), F32),
            pltpu.VMEM((replicas, 2, listed, LISTED), F32),
            pltpu.VMEM((parts, 8, QUAD), F32),
            pltpu.SemaphoreType.DMA((6,)),
            pltpu.SemaphoreType.DMA((replicas,)),
            pltpu.SemaphoreType.DMA((replicas,)),
            pltpu.SemaphoreType.DMA((parts,)),
            pltpu.SemaphoreType.DMA((parts,)),
        ],
        compiler_params=pltpu.CompilerParams(
            collective_id=0, has_side_effects=True, vmem_limit_bytes=24 * 1024 * 1024
        ),
    )(
        *(
            pltpu.with_memory_space_constraint(array, pltpu.HBM)
            for array in (
                gradient, momentum, weights, jnp.swapaxes(positions, 2, 3),
                jnp.asarray(row_tables), jnp.asarray(column_tables),
            )
        )
    )
    return pl.pallas_call(
        deliver,
        out_shape=(
            jax.ShapeDtypeStruct(momentum.shape, F32),
            jax.ShapeDtypeStruct(weights.shape, F32),
        ),
        in_specs=[vmem] * 2,
        out_specs=(anywhere, anywhere),
        scratch_shapes=[pltpu.SemaphoreType.DMA((2,))],
        compiler_params=pltpu.CompilerParams(vmem_limit_bytes=8 * 1024 * 1024),
    )(*results)


def solution(mesh):
    placed = (P("dp", None, "mp"), P("dp", None, "mp"), P(None, "mp"), P("dp", None, "mp", None))
    return jax.shard_map(
        functools.partial(local, mesh.shape["dp"], mesh.shape["mp"]),
        mesh=mesh,
        in_specs=placed,
        out_specs=(P("dp", None, "mp"), P(None, "mp")),
        check_vma=False,
    )
```

```python
import functools

import jax
import jax.numpy as jnp
import numpy as np
from jax import lax
from jax.experimental import pallas as pl
from jax.experimental.pallas import tpu as pltpu
from jax.sharding import PartitionSpec as P

QUAD = 256
PAIR = 128
GROUP = 8
F32 = jnp.float32
BF16 = jnp.bfloat16


def dct_table():
    column = np.arange(64, dtype=np.float64)
    freq = column[:, None]
    factor = np.where(freq == 0, np.sqrt(1.0 / 64), np.sqrt(2.0 / 64))
    return factor * np.cos(np.pi * (2.0 * column[None, :] + 1.0) * freq / 128.0)


def halves(table):
    high = np.asarray(table, np.float32).astype(jnp.bfloat16)
    low = np.asarray(table - high.astype(np.float64), np.float32).astype(jnp.bfloat16)
    return high, low


def side_tables():
    table = dct_table()
    rows, columns = [], []
    for row, column in ((table, table.T), (table.T, table)):
        high, low = halves(row)
        rows.append(np.concatenate([high, low, high, low], axis=1))
        columns.append(np.concatenate(halves(np.kron(np.eye(2), column)), axis=1))
    return np.stack(rows), np.stack(columns)


def split(value):
    high = value.astype(BF16)
    return high, (value - high.astype(F32)).astype(BF16)


def dot(a, b):
    return jnp.dot(a, b, preferred_element_type=F32)


def dot_t(a, b):
    return lax.dot_general(a, b, (((1,), (1,)), ((), ())), preferred_element_type=F32)


def row_transform(table, value):
    high, low = split(value)
    return dot(table, jnp.concatenate([high, high, low, low], axis=0))


def column_transform(both, table):
    result = dot(both, jnp.concatenate([table, table], axis=0))
    return result[:, :PAIR] + result[:, PAIR:]


def counting(rows, lanes):
    count = lax.broadcasted_iota(jnp.int32, (rows, lanes), 0).astype(F32)
    return count.astype(BF16).reshape(-1, 16, lanes)


def spread(row):
    return jnp.broadcast_to(row, (16, row.shape[1])).astype(BF16)[None]


def flat(tiles):
    return tiles.reshape(-1, tiles.shape[-1])


def frequencies(places):
    return (places // 64).astype(F32), (places % 64).astype(F32)


def lane_part(shape):
    return lax.broadcasted_iota(jnp.int32, shape, 1) // 32


def regroup(members, part):
    result = []
    for start in range(0, GROUP, 4):
        joined = None
        for place in range(4):
            member = members[start + place]
            shift = (place - part) % 4 * 32
            moved = pltpu.roll(member, shift, axis=1) if shift else member
            joined = moved if joined is None else jnp.where(lane_part(moved.shape) == place, moved, joined)
        result.append(joined)
    return jnp.concatenate(result, axis=1)


def loop(count, body):
    if count <= 16:
        for step in range(count):
            body(step)
    else:
        lax.fori_loop(0, count, lambda step, carry: (body(step), carry)[1], 0)


def kernel(
    replicas, parts, entries,
    gradient_ref, momentum_ref, weights_ref, places_hbm, rows_hbm, columns_hbm,
    summed, update,
    grad, mom, wts, places_ref, rows_ref, columns_ref, flipped, both, coefs,
    place_lists, value_lists, row_parts, column_parts, value_parts, squares,
    in_sem, place_send, place_recv, value_send, value_recv, square_send, square_recv,
):
    me, mine = lax.axis_index("dp"), lax.axis_index("mp")
    width = summed.shape[1]
    quads = width // QUAD

    loads = [
        pltpu.make_async_copy(source, target, in_sem.at[index])
        for index, (source, target) in enumerate(
            (
                (places_hbm.at[0, 0], places_ref), (rows_hbm, rows_ref), (gradient_ref.at[0], grad),
                (momentum_ref.at[0], mom), (columns_hbm, columns_ref), (weights_ref, wts),
            )
        )
    ]
    barrier = pltpu.get_barrier_semaphore()

    def greet_replica(step):
        pl.semaphore_signal(
            barrier, inc=1, device_id={"dp": lax.rem(me + step + 1, replicas)},
            device_id_type=pl.DeviceIdType.MESH,
        )

    def greet_part(step):
        pl.semaphore_signal(
            barrier, inc=1, device_id={"mp": lax.rem(mine + step + 1, parts)},
            device_id_type=pl.DeviceIdType.MESH,
        )

    loop(replicas - 1, greet_replica)
    loop(parts - 1, greet_part)
    for load in loads:
        load.start()

    def block(index):
        return pl.ds(index * QUAD, QUAD)

    def rows(index):
        return pl.ds(index * 64, 64)

    def quad(ref, index):
        return jnp.concatenate([ref[rows(2 * index), :], ref[rows(2 * index + 1), :]], axis=1)

    def keep(index, value):
        for half, part in enumerate(split(value)):
            for side in range(2):
                both[rows(2 * index + side), half * PAIR : (half + 1) * PAIR] = part[
                    :, side * PAIR : (side + 1) * PAIR
                ]

    def keep_pair(index, value):
        for half, part in enumerate(split(value)):
            both[rows(index), half * PAIR : (half + 1) * PAIR] = part

    def list_copy(lists, send_sem, recv_sem, step, slot):
        return pltpu.make_async_remote_copy(
            src_ref=lists.at[slot], dst_ref=lists.at[slot],
            send_sem=send_sem.at[step], recv_sem=recv_sem.at[slot],
            device_id={"dp": lax.rem(me + step + 1, replicas)},
            device_id_type=pl.DeviceIdType.MESH,
        )

    def place_copy(step, slot):
        return list_copy(place_lists, place_send, place_recv, step, slot)

    def value_copy(step, slot):
        return list_copy(value_lists, value_send, value_recv, step, slot)

    groups = place_lists.shape[0] // GROUP
    for slot in range(replicas, groups * GROUP):
        place_lists[slot, :, :] = jnp.zeros(place_lists.shape[1:], F32)
        value_lists[slot, :, :] = jnp.zeros(value_lists.shape[1:], F32)

    loads[0].wait()
    flipped[...] = jnp.transpose(places_ref[...])
    places = jnp.concatenate(
        [flipped[pl.ds(part, quads, stride=4), :] for part in range(4)], axis=1
    )
    place_lists[me, 0:quads, :] = places.astype(F32)

    for load in loads[1:4]:
        load.wait()
    for index in range(quads):
        value = 0.9 * mom[:, block(index)] + grad[:, block(index)].astype(F32)
        summed[:, block(index)] = value
        keep(index, row_transform(rows_ref[0], value))

    pl.semaphore_wait(barrier, replicas - 1 + parts - 1)
    loop(replicas - 1, lambda step: place_copy(step, me).start())

    loads[4].wait()
    coefs[...] = column_transform(both[...], columns_ref[0])

    zero, one = jnp.zeros((), BF16), jnp.ones((), BF16)
    count_quad = counting(QUAD, PAIR)
    row_freqs, spots = frequencies(places)
    spots = spots + (lane_part(places.shape) * 64).astype(F32)
    for index in range(quads):
        row_hot = flat(jnp.where(count_quad[:4] == spread(row_freqs[index : index + 1, :]), one, zero))
        column_hot = flat(jnp.where(count_quad == spread(spots[index : index + 1, :]), one, zero))
        value = quad(coefs, index)
        found = dot(jnp.concatenate(split(value), axis=0), column_hot)
        found = (found[:64, :] + found[64:, :]) * row_hot.astype(F32)
        value_lists[me, index : index + 1, :] = jnp.sum(found, axis=0, keepdims=True)
        keep(index, value * dot_t(row_hot, column_hot))

    loop(replicas - 1, lambda step: value_copy(step, me).start())

    coefs[...] = column_transform(both[...], columns_ref[1])
    for index in range(quads):
        back = row_transform(rows_ref[1], quad(coefs, index))
        summed[:, block(index)] = summed[:, block(index)] - back

    def source(step):
        return lax.rem(me + replicas - step - 1, replicas)

    def regroup_places(group):
        members = [
            frequencies(place_lists[group * GROUP + member, :, :].astype(jnp.int32))
            for member in range(GROUP)
        ]
        for part in range(4):
            row_parts[group, part, :, :] = regroup([member[0] for member in members], part)
            column_parts[group, part, :, :] = regroup([member[1] for member in members], part)

    def regroup_values(group):
        members = [value_lists[group * GROUP + member, :, :] for member in range(GROUP)]
        for part in range(4):
            value_parts[group, part, :, :] = regroup(members, part)

    loop(replicas - 1, lambda step: place_copy(step, source(step)).wait_recv())
    loop(groups, regroup_places)
    loop(replicas - 1, lambda step: value_copy(step, source(step)).wait_recv())
    loop(groups, regroup_values)

    count_group = counting(64, GROUP * 32)

    def decode(group, index, part):
        line = slice(index, index + 1)
        row_hot = flat(jnp.where(count_group == spread(row_parts[group, part, line, :]), one, zero))
        here = count_group == spread(column_parts[group, part, line, :])
        high, low = split(jnp.broadcast_to(value_parts[group, part, line, :], (16, GROUP * 32)))
        right = jnp.concatenate(
            [flat(jnp.where(here, high[None], zero)), flat(jnp.where(here, low[None], zero))], axis=0
        )
        result = dot_t(row_hot, right)
        return result + pltpu.roll(result, 64, axis=1)

    def decode_pair(group, index, side):
        left, right = (decode(group, index, 2 * side + place) for place in range(2))
        return jnp.where(lane_part(left.shape) < 2, left, right)

    square = jnp.zeros((8, PAIR), F32)
    for index in range(quads):
        for side in range(2):
            total = decode_pair(0, index, side)
            if groups > 1:
                total = lax.fori_loop(
                    1, groups, lambda step, acc: acc + decode_pair(step, index, side), total
                )
            square = square + jnp.sum((total * total).reshape(8, 8, PAIR), axis=0)
            keep_pair(2 * index + side, total)

    squares[mine, :, :] = square

    def square_copy(step, slot):
        return pltpu.make_async_remote_copy(
            src_ref=squares.at[slot], dst_ref=squares.at[slot],
            send_sem=square_send.at[step], recv_sem=square_recv.at[slot],
            device_id={"mp": lax.rem(mine + step + 1, parts)},
            device_id_type=pl.DeviceIdType.MESH,
        )

    loop(parts - 1, lambda step: square_copy(step, mine).start())

    coefs[...] = column_transform(both[...], columns_ref[1])
    for index in range(quads):
        update[:, block(index)] = row_transform(rows_ref[1], quad(coefs, index))

    loop(
        parts - 1,
        lambda step: square_copy(step, lax.rem(mine + parts - step - 1, parts)).wait_recv(),
    )
    loads[5].wait()
    meansq = jnp.sum(jnp.sum(squares[...], axis=0)) / entries
    factor = lax.rsqrt(jnp.full((1, QUAD), meansq + 1.0, F32))
    for index in range(quads):
        update[:, block(index)] = wts[:, block(index)] - update[:, block(index)] * factor
    loop(replicas - 1, lambda step: place_copy(step, me).wait_send())
    loop(replicas - 1, lambda step: value_copy(step, me).wait_send())
    loop(parts - 1, lambda step: square_copy(step, mine).wait_send())


def deliver(summed, update, out_momentum_ref, out_weights_ref, out_sem):
    stores = (
        pltpu.make_async_copy(summed, out_momentum_ref.at[0], out_sem.at[0]),
        pltpu.make_async_copy(update, out_weights_ref, out_sem.at[1]),
    )
    for store in stores:
        store.start()
    for store in stores:
        store.wait()


def local(replicas, parts, gradient, momentum, weights, positions):
    height, width = weights.shape
    quads = width // QUAD
    row_tables, column_tables = side_tables()
    anywhere = pl.BlockSpec(memory_space=pl.ANY)
    vmem = pl.BlockSpec(memory_space=pltpu.VMEM)
    listed = -(-quads // 8) * 8
    groups = -(-replicas // GROUP)
    entries = positions.shape[-1]
    results = pl.pallas_call(
        functools.partial(kernel, replicas, parts, float(height * width * parts)),
        out_shape=(
            jax.ShapeDtypeStruct(weights.shape, F32),
            jax.ShapeDtypeStruct(weights.shape, F32),
        ),
        in_specs=[pl.BlockSpec(memory_space=pltpu.HBM)] * 6,
        out_specs=(vmem, vmem),
        scratch_shapes=[
            pltpu.VMEM((height, width), BF16),
            pltpu.VMEM((height, width), F32),
            pltpu.VMEM((height, width), F32),
            pltpu.VMEM((entries, 4 * quads), jnp.int32),
            pltpu.VMEM(row_tables.shape, BF16),
            pltpu.VMEM(column_tables.shape, BF16),
            pltpu.VMEM((4 * quads, entries), jnp.int32),
            pltpu.VMEM((2 * quads * 64, QUAD), BF16),
            pltpu.VMEM((2 * quads * 64, PAIR), F32),
            pltpu.VMEM((groups * GROUP, listed, PAIR), F32),
            pltpu.VMEM((groups * GROUP, listed, PAIR), F32),
            pltpu.VMEM((groups, 4, listed, GROUP * 32), F32),
            pltpu.VMEM((groups, 4, listed, GROUP * 32), F32),
            pltpu.VMEM((groups, 4, listed, GROUP * 32), F32),
            pltpu.VMEM((parts, 8, PAIR), F32),
            pltpu.SemaphoreType.DMA((6,)),
            pltpu.SemaphoreType.DMA((replicas,)),
            pltpu.SemaphoreType.DMA((replicas,)),
            pltpu.SemaphoreType.DMA((replicas,)),
            pltpu.SemaphoreType.DMA((replicas,)),
            pltpu.SemaphoreType.DMA((parts,)),
            pltpu.SemaphoreType.DMA((parts,)),
        ],
        compiler_params=pltpu.CompilerParams(
            collective_id=0, has_side_effects=True, vmem_limit_bytes=24 * 1024 * 1024
        ),
    )(
        *(
            pltpu.with_memory_space_constraint(array, pltpu.HBM)
            for array in (
                gradient, momentum, weights, jnp.swapaxes(positions, 2, 3),
                jnp.asarray(row_tables), jnp.asarray(column_tables),
            )
        )
    )
    return pl.pallas_call(
        deliver,
        out_shape=(
            jax.ShapeDtypeStruct(momentum.shape, F32),
            jax.ShapeDtypeStruct(weights.shape, F32),
        ),
        in_specs=[vmem] * 2,
        out_specs=(anywhere, anywhere),
        scratch_shapes=[pltpu.SemaphoreType.DMA((2,))],
        compiler_params=pltpu.CompilerParams(vmem_limit_bytes=8 * 1024 * 1024),
    )(*results)


def solution(mesh):
    placed = (P("dp", None, "mp"), P("dp", None, "mp"), P(None, "mp"), P("dp", None, "mp", None))
    return jax.shard_map(
        functools.partial(local, mesh.shape["dp"], mesh.shape["mp"]),
        mesh=mesh,
        in_specs=placed,
        out_specs=(P("dp", None, "mp"), P(None, "mp")),
        check_vma=False,
    )
```

```python
import functools

import jax
import jax.numpy as jnp
import numpy as np
from jax import lax
from jax.experimental import pallas as pl
from jax.experimental.pallas import tpu as pltpu
from jax.sharding import PartitionSpec as P

QUAD = 256
PAIR = 128
GROUP = 8
CHUNKS = 4
F32 = jnp.float32
BF16 = jnp.bfloat16


def dct_table():
    column = np.arange(64, dtype=np.float64)
    freq = column[:, None]
    factor = np.where(freq == 0, np.sqrt(1.0 / 64), np.sqrt(2.0 / 64))
    return factor * np.cos(np.pi * (2.0 * column[None, :] + 1.0) * freq / 128.0)


def halves(table):
    high = np.asarray(table, np.float32).astype(jnp.bfloat16)
    low = np.asarray(table - high.astype(np.float64), np.float32).astype(jnp.bfloat16)
    return high, low


def side_tables():
    table = dct_table()
    rows, columns = [], []
    for row, column in ((table, table.T), (table.T, table)):
        high, low = halves(row)
        rows.append(np.concatenate([high, low, high, low], axis=1))
        columns.append(np.concatenate(halves(np.kron(np.eye(2), column)), axis=1))
    return np.stack(rows), np.stack(columns)


def split(value):
    high = value.astype(BF16)
    return high, (value - high.astype(F32)).astype(BF16)


def dot(a, b):
    return jnp.dot(a, b, preferred_element_type=F32)


def dot_t(a, b):
    return lax.dot_general(a, b, (((1,), (1,)), ((), ())), preferred_element_type=F32)


def row_transform(table, value):
    high, low = split(value)
    return dot(table, jnp.concatenate([high, high, low, low], axis=0))


def column_transform(both, table):
    result = dot(both, jnp.concatenate([table, table], axis=0))
    return result[:, :PAIR] + result[:, PAIR:]


def counting(rows, lanes):
    count = lax.broadcasted_iota(jnp.int32, (rows, lanes), 0).astype(F32)
    return count.astype(BF16).reshape(-1, 16, lanes)


def spread(row):
    return jnp.broadcast_to(row, (16, row.shape[1])).astype(BF16)[None]


def flat(tiles):
    return tiles.reshape(-1, tiles.shape[-1])


def frequencies(places):
    return (places // 64).astype(F32), (places % 64).astype(F32)


def lane_part(shape):
    return lax.broadcasted_iota(jnp.int32, shape, 1) // 32


def regroup(members, part):
    result = []
    for start in range(0, GROUP, 4):
        joined = None
        for place in range(4):
            member = members[start + place]
            shift = (place - part) % 4 * 32
            moved = pltpu.roll(member, shift, axis=1) if shift else member
            joined = moved if joined is None else jnp.where(lane_part(moved.shape) == place, moved, joined)
        result.append(joined)
    return jnp.concatenate(result, axis=1)


def loop(count, body):
    if count <= 16:
        for step in range(count):
            body(step)
    else:
        lax.fori_loop(0, count, lambda step, carry: (body(step), carry)[1], 0)


def kernel(
    replicas, parts, entries,
    gradient_ref, momentum_ref, weights_ref, places_hbm, rows_hbm, columns_hbm,
    summed, update,
    grad, mom, wts, places_ref, rows_ref, columns_ref, flipped, both, coefs,
    place_lists, value_lists, row_parts, column_parts, value_parts, squares,
    in_sem, chunk_sem, place_send, place_recv, value_send, value_recv, square_send, square_recv,
):
    me, mine = lax.axis_index("dp"), lax.axis_index("mp")
    width = summed.shape[1]
    quads = width // QUAD

    loads = [
        pltpu.make_async_copy(source, target, in_sem.at[index])
        for index, (source, target) in enumerate(
            (
                (places_hbm.at[0, 0], places_ref), (rows_hbm, rows_ref),
                (columns_hbm, columns_ref), (weights_ref, wts),
            )
        )
    ]
    stride = -(-quads // CHUNKS) * QUAD
    chunks = []
    for index, start in enumerate(range(0, width, stride)):
        some = slice(start, min(start + stride, width))
        chunks.append((
            pltpu.make_async_copy(gradient_ref.at[0, :, some], grad.at[:, some], chunk_sem.at[0, index]),
            pltpu.make_async_copy(momentum_ref.at[0, :, some], mom.at[:, some], chunk_sem.at[1, index]),
        ))
    barrier = pltpu.get_barrier_semaphore()

    def greet_replica(step):
        pl.semaphore_signal(
            barrier, inc=1, device_id={"dp": lax.rem(me + step + 1, replicas)},
            device_id_type=pl.DeviceIdType.MESH,
        )

    def greet_part(step):
        pl.semaphore_signal(
            barrier, inc=1, device_id={"mp": lax.rem(mine + step + 1, parts)},
            device_id_type=pl.DeviceIdType.MESH,
        )

    loop(replicas - 1, greet_replica)
    loop(parts - 1, greet_part)
    for load in loads[:2]:
        load.start()
    for chunk in chunks:
        for load in chunk:
            load.start()
    for load in loads[2:]:
        load.start()

    def block(index):
        return pl.ds(index * QUAD, QUAD)

    def rows(index):
        return pl.ds(index * 64, 64)

    def quad(ref, index):
        return jnp.concatenate([ref[rows(2 * index), :], ref[rows(2 * index + 1), :]], axis=1)

    def keep(index, value):
        for half, part in enumerate(split(value)):
            for side in range(2):
                both[rows(2 * index + side), half * PAIR : (half + 1) * PAIR] = part[
                    :, side * PAIR : (side + 1) * PAIR
                ]

    def keep_pair(index, value):
        for half, part in enumerate(split(value)):
            both[rows(index), half * PAIR : (half + 1) * PAIR] = part

    def list_copy(lists, send_sem, recv_sem, step, slot):
        return pltpu.make_async_remote_copy(
            src_ref=lists.at[slot], dst_ref=lists.at[slot],
            send_sem=send_sem.at[step], recv_sem=recv_sem.at[slot],
            device_id={"dp": lax.rem(me + step + 1, replicas)},
            device_id_type=pl.DeviceIdType.MESH,
        )

    def place_copy(step, slot):
        return list_copy(place_lists, place_send, place_recv, step, slot)

    def value_copy(step, slot):
        return list_copy(value_lists, value_send, value_recv, step, slot)

    groups = place_lists.shape[0] // GROUP
    for slot in range(replicas, groups * GROUP):
        place_lists[slot, :, :] = jnp.zeros(place_lists.shape[1:], F32)
        value_lists[slot, :, :] = jnp.zeros(value_lists.shape[1:], F32)

    loads[0].wait()
    flipped[...] = jnp.transpose(places_ref[...])
    places = jnp.concatenate(
        [flipped[pl.ds(part, quads, stride=4), :] for part in range(4)], axis=1
    )
    place_lists[me, 0:quads, :] = places.astype(F32)

    loads[1].wait()
    for index in range(quads):
        if index * QUAD % stride == 0:
            for load in chunks[index * QUAD // stride]:
                load.wait()
        value = 0.9 * mom[:, block(index)] + grad[:, block(index)].astype(F32)
        summed[:, block(index)] = value
        keep(index, row_transform(rows_ref[0], value))

    pl.semaphore_wait(barrier, replicas - 1 + parts - 1)
    loop(replicas - 1, lambda step: place_copy(step, me).start())

    loads[2].wait()
    coefs[...] = column_transform(both[...], columns_ref[0])

    zero, one = jnp.zeros((), BF16), jnp.ones((), BF16)
    count_quad = counting(QUAD, PAIR)
    row_freqs, spots = frequencies(places)
    spots = spots + (lane_part(places.shape) * 64).astype(F32)
    for index in range(quads):
        row_hot = flat(jnp.where(count_quad[:4] == spread(row_freqs[index : index + 1, :]), one, zero))
        column_hot = flat(jnp.where(count_quad == spread(spots[index : index + 1, :]), one, zero))
        value = quad(coefs, index)
        found = dot(jnp.concatenate(split(value), axis=0), column_hot)
        found = (found[:64, :] + found[64:, :]) * row_hot.astype(F32)
        value_lists[me, index : index + 1, :] = jnp.sum(found, axis=0, keepdims=True)
        keep(index, value * dot_t(row_hot, column_hot))

    loop(replicas - 1, lambda step: value_copy(step, me).start())

    coefs[...] = column_transform(both[...], columns_ref[1])
    for index in range(quads):
        back = row_transform(rows_ref[1], quad(coefs, index))
        summed[:, block(index)] = summed[:, block(index)] - back

    def source(step):
        return lax.rem(me + replicas - step - 1, replicas)

    def regroup_places(group):
        members = [
            frequencies(place_lists[group * GROUP + member, :, :].astype(jnp.int32))
            for member in range(GROUP)
        ]
        for part in range(4):
            row_parts[group, part, :, :] = regroup([member[0] for member in members], part)
            column_parts[group, part, :, :] = regroup([member[1] for member in members], part)

    def regroup_values(group):
        members = [value_lists[group * GROUP + member, :, :] for member in range(GROUP)]
        for part in range(4):
            value_parts[group, part, :, :] = regroup(members, part)

    loop(replicas - 1, lambda step: place_copy(step, source(step)).wait_recv())
    loop(groups, regroup_places)
    loop(replicas - 1, lambda step: value_copy(step, source(step)).wait_recv())
    loop(groups, regroup_values)

    count_group = counting(64, GROUP * 32)

    def decode(group, index, part):
        line = slice(index, index + 1)
        row_hot = flat(jnp.where(count_group == spread(row_parts[group, part, line, :]), one, zero))
        here = count_group == spread(column_parts[group, part, line, :])
        high, low = split(jnp.broadcast_to(value_parts[group, part, line, :], (16, GROUP * 32)))
        right = jnp.concatenate(
            [flat(jnp.where(here, high[None], zero)), flat(jnp.where(here, low[None], zero))], axis=0
        )
        result = dot_t(row_hot, right)
        return result + pltpu.roll(result, 64, axis=1)

    def decode_pair(group, index, side):
        left, right = (decode(group, index, 2 * side + place) for place in range(2))
        return jnp.where(lane_part(left.shape) < 2, left, right)

    square = jnp.zeros((8, PAIR), F32)
    for index in range(quads):
        for side in range(2):
            total = decode_pair(0, index, side)
            if groups > 1:
                total = lax.fori_loop(
                    1, groups, lambda step, acc: acc + decode_pair(step, index, side), total
                )
            square = square + jnp.sum((total * total).reshape(8, 8, PAIR), axis=0)
            keep_pair(2 * index + side, total)

    squares[mine, :, :] = square

    def square_copy(step, slot):
        return pltpu.make_async_remote_copy(
            src_ref=squares.at[slot], dst_ref=squares.at[slot],
            send_sem=square_send.at[step], recv_sem=square_recv.at[slot],
            device_id={"mp": lax.rem(mine + step + 1, parts)},
            device_id_type=pl.DeviceIdType.MESH,
        )

    loop(parts - 1, lambda step: square_copy(step, mine).start())

    coefs[...] = column_transform(both[...], columns_ref[1])
    for index in range(quads):
        update[:, block(index)] = row_transform(rows_ref[1], quad(coefs, index))

    loop(
        parts - 1,
        lambda step: square_copy(step, lax.rem(mine + parts - step - 1, parts)).wait_recv(),
    )
    loads[3].wait()
    meansq = jnp.sum(jnp.sum(squares[...], axis=0)) / entries
    factor = lax.rsqrt(jnp.full((1, QUAD), meansq + 1.0, F32))
    for index in range(quads):
        update[:, block(index)] = wts[:, block(index)] - update[:, block(index)] * factor
    loop(replicas - 1, lambda step: place_copy(step, me).wait_send())
    loop(replicas - 1, lambda step: value_copy(step, me).wait_send())
    loop(parts - 1, lambda step: square_copy(step, mine).wait_send())


def deliver(summed, update, out_momentum_ref, out_weights_ref, out_sem):
    share = summed.shape[0] // CHUNKS
    stores = []
    for index in range(CHUNKS):
        some = pl.ds(index * share, share)
        stores.append(pltpu.make_async_copy(summed.at[some], out_momentum_ref.at[0, some], out_sem.at[0, index]))
        stores.append(pltpu.make_async_copy(update.at[some], out_weights_ref.at[some], out_sem.at[1, index]))
    for store in stores:
        store.start()
    for store in stores:
        store.wait()


def local(replicas, parts, gradient, momentum, weights, positions):
    height, width = weights.shape
    quads = width // QUAD
    row_tables, column_tables = side_tables()
    anywhere = pl.BlockSpec(memory_space=pl.ANY)
    vmem = pl.BlockSpec(memory_space=pltpu.VMEM)
    listed = -(-quads // 8) * 8
    groups = -(-replicas // GROUP)
    entries = positions.shape[-1]
    results = pl.pallas_call(
        functools.partial(kernel, replicas, parts, float(height * width * parts)),
        out_shape=(
            jax.ShapeDtypeStruct(weights.shape, F32),
            jax.ShapeDtypeStruct(weights.shape, F32),
        ),
        in_specs=[pl.BlockSpec(memory_space=pltpu.HBM)] * 6,
        out_specs=(vmem, vmem),
        scratch_shapes=[
            pltpu.VMEM((height, width), BF16),
            pltpu.VMEM((height, width), F32),
            pltpu.VMEM((height, width), F32),
            pltpu.VMEM((entries, 4 * quads), jnp.int32),
            pltpu.VMEM(row_tables.shape, BF16),
            pltpu.VMEM(column_tables.shape, BF16),
            pltpu.VMEM((4 * quads, entries), jnp.int32),
            pltpu.VMEM((2 * quads * 64, QUAD), BF16),
            pltpu.VMEM((2 * quads * 64, PAIR), F32),
            pltpu.VMEM((groups * GROUP, listed, PAIR), F32),
            pltpu.VMEM((groups * GROUP, listed, PAIR), F32),
            pltpu.VMEM((groups, 4, listed, GROUP * 32), F32),
            pltpu.VMEM((groups, 4, listed, GROUP * 32), F32),
            pltpu.VMEM((groups, 4, listed, GROUP * 32), F32),
            pltpu.VMEM((parts, 8, PAIR), F32),
            pltpu.SemaphoreType.DMA((4,)),
            pltpu.SemaphoreType.DMA((2, CHUNKS)),
            pltpu.SemaphoreType.DMA((replicas,)),
            pltpu.SemaphoreType.DMA((replicas,)),
            pltpu.SemaphoreType.DMA((replicas,)),
            pltpu.SemaphoreType.DMA((replicas,)),
            pltpu.SemaphoreType.DMA((parts,)),
            pltpu.SemaphoreType.DMA((parts,)),
        ],
        compiler_params=pltpu.CompilerParams(
            collective_id=0, has_side_effects=True, vmem_limit_bytes=24 * 1024 * 1024
        ),
    )(
        *(
            pltpu.with_memory_space_constraint(array, pltpu.HBM)
            for array in (
                gradient, momentum, weights, jnp.swapaxes(positions, 2, 3),
                jnp.asarray(row_tables), jnp.asarray(column_tables),
            )
        )
    )
    return pl.pallas_call(
        deliver,
        out_shape=(
            jax.ShapeDtypeStruct(momentum.shape, F32),
            jax.ShapeDtypeStruct(weights.shape, F32),
        ),
        in_specs=[vmem] * 2,
        out_specs=(anywhere, anywhere),
        scratch_shapes=[pltpu.SemaphoreType.DMA((2, CHUNKS))],
        compiler_params=pltpu.CompilerParams(vmem_limit_bytes=8 * 1024 * 1024),
    )(*results)


def solution(mesh):
    placed = (P("dp", None, "mp"), P("dp", None, "mp"), P(None, "mp"), P("dp", None, "mp", None))
    return jax.shard_map(
        functools.partial(local, mesh.shape["dp"], mesh.shape["mp"]),
        mesh=mesh,
        in_specs=placed,
        out_specs=(P("dp", None, "mp"), P(None, "mp")),
        check_vma=False,
    )
```
